32 devices in a mesh: dp: 4 (over y, x), vocab: 8 (over z, core).
Axes of the slice: x: 2, y: 2, z: 4, core: 2. Of those that a mesh axis runs over, the one named last changes fastest.
Arguments:
- hidden: bfloat16 [256, 4096], P('dp'), may hold values from -0.75 to 0.75
- head_weight: bfloat16 [4096, 128256], P(None, ('dp', 'vocab')), may hold values from -0.75 to 0.75
- target_ids: int32 [256], P('dp'), may hold values from 0 to 128255
- loss_mask: int32 [256], P('dp'), may hold values from 0 to 1, as said below
- doc_ids: int32 [256], P('dp'), may hold values from 0 to 31, as said below
- loss_scale: float32 [], replicated, may hold values from 512 to 2048
Outputs:
- mean_loss: float32 [], replicated
- head_grad: bfloat16 [4096, 128256], P(None, ('dp', 'vocab'))
- hidden_grad: bfloat16 [256, 4096], P(None, ('dp', 'vocab'))
The draws below stay inside these ranges and needn't reach their ends.
Inputs may be any that keep to these rules, and one draw needn't show every extreme that they name: loss_mask is 0 or 1; among the 64 positions of each data group (aligned blocks of 64 positions) at most 32 have loss_mask 1, and exactly 32 in one of them; the last position of each data group has loss_mask 1. doc_ids starts at 0 and never falls; from one position to the next it grows by 0 or 1; its last value is 31.
All inputs are finite; a program needn't handle non-finite values.
Results may differ from the reference program's by a relative error of at most 0.0017.
Values may be sent and summed in bfloat16 or wider, within the bound.
A program may use at most 128 MiB of HBM per device.

```python
import math
import jax
import jax.numpy as jnp
import numpy as np
from jax import lax

D = 4096
V = 128256
TOK_DEV = 64
TOKENS = 256
VALID_MOST = 32
N_DP = 4
N_VOCAB = 8


def draw_loss_mask(key, part):
    groups = TOKENS // TOK_DEV
    first_key, second_key, third_key = jax.random.split(key, 3)
    busiest = jax.random.randint(first_key, (), 0, groups)
    counts = jax.random.randint(second_key, (groups,), TOK_DEV // 16, TOK_DEV // 4 + 1)
    counts = jnp.where(jnp.arange(groups) == busiest, VALID_MOST, counts)
    orders = jax.vmap(lambda sub_key: jax.random.permutation(sub_key, TOK_DEV - 1))(jax.random.split(third_key, groups))
    chosen = (orders < (counts - 1)[:, None]).astype(jnp.int32)
    chosen = jnp.concatenate([chosen, jnp.ones((groups, 1), jnp.int32)], axis=1)
    return chosen.reshape(TOKENS)


def draw_doc_ids(key, part):
    order_key = jax.random.fold_in(key, 7)
    orders = jax.random.permutation(order_key, TOKENS - 1)
    flags = (orders < TOKENS // 8 - 1).astype(jnp.int32)
    starts = jnp.concatenate([jnp.zeros((1,), jnp.int32), flags])
    return jnp.cumsum(starts).astype(jnp.int32)


def set_ends(entries, own_key, low, high):
    index_at = [jax.random.randint(jax.random.fold_in(own_key, axis), (), 0, length) for axis, length in enumerate(entries.shape)]
    widest = entries.shape.index(max(entries.shape))
    next_to = index_at[:widest] + [(index_at[widest] + 1) % entries.shape[widest]] + index_at[widest + 1:]
    return entries.at[tuple(index_at)].set(low).at[tuple(next_to)].set(high)


def block_levels(own_key, dims, shards, least, largest):
    factor_of = 1.0
    for position, shards_of in shards:
        draws = jax.random.uniform(jax.random.fold_in(jax.random.fold_in(own_key, 6), position), (shards_of,), jnp.float32, least / len(shards), largest / len(shards))
        factor_of = factor_of * jnp.repeat(jnp.exp(draws), dims[position] // shards_of).reshape((-1,) + (1,) * (len(dims) - 1 - position))
    return factor_of


def ranked_wide(stream_key, extent, number_of, lean):
    weights = [min(1 << octave, number_of + 1 - (1 << octave)) * (1 << 20) // math.isqrt((1 << octave) ** lean) + 1 for octave in range((number_of + 1).bit_length()) if 1 << octave <= number_of]
    spread = 1 + sum(weights) // (1 << 30)
    listing = np.cumsum(np.array([max(1, weight // spread) for weight in weights]))
    ticket = jax.random.randint(jax.random.fold_in(stream_key, 1), extent, 0, int(listing[len(weights) - 1]))
    start = jnp.left_shift(1, jnp.searchsorted(jnp.asarray(listing, jnp.int32), ticket, side="right").astype(jnp.int32))
    grade = start - 1 + jax.random.randint(jax.random.fold_in(stream_key, 4), extent, 0, 1 << 30) % jnp.minimum(start, number_of + 1 - start)
    return jax.random.permutation(jax.random.fold_in(stream_key, 2), number_of)[grade].astype(jnp.int32)


def normal_values(own_key, dims, spread, reach, shards=(), kind=jnp.bfloat16):
    factor_of = block_levels(own_key, dims, shards, -0.22, 0.18) if shards else 1.0
    entries = jax.random.normal(own_key, dims, jnp.float32) * spread * factor_of
    return jnp.minimum(jnp.maximum(entries, -reach), reach).astype(kind)


def setup_inputs(seed: int = 0) -> dict:
    splits = jax.random.split(jax.random.key(seed), 7)
    hidden = normal_values(splits[0], (TOKENS, D), (D ** -0.25), 0.75, ((0, 4),))
    head_weight = normal_values(splits[1], (D, V), (D ** 0.5) ** -0.5, 0.75, ((1, 32),))
    target_ids = set_ends(ranked_wide(splits[2], (TOKENS,), V, 2), jax.random.fold_in(splits[2], 3), 0, V - 1).astype(jnp.int32)
    loss_mask = draw_loss_mask(jax.random.fold_in(splits[6], 71), 0)
    doc_ids = draw_doc_ids(jax.random.fold_in(splits[6], 71), 0)
    loss_scale = jnp.clip(jnp.exp(jax.random.uniform(splits[5], (), jnp.float32, math.log(512.0), math.log(2048.0))), 512.0, 2048.0)
    return {"hidden": hidden, "head_weight": head_weight, "target_ids": target_ids, "loss_mask": loss_mask, "doc_ids": doc_ids, "loss_scale": loss_scale}


def reference(hidden, head_weight, target_ids, loss_mask, doc_ids, loss_scale):
    following = jnp.concatenate([doc_ids[1:], jnp.full((1,), -1, jnp.int32)])
    valid_rows = loss_mask * (following == doc_ids).astype(jnp.int32)
    weight_rows = valid_rows.astype(jnp.float32)
    blocks = N_DP * N_VOCAB
    block_cols = V // blocks
    logits = jnp.dot(hidden, head_weight, preferred_element_type=jnp.float32)
    row_max = lax.optimization_barrier(jnp.max(logits, axis=1))
    log_total = row_max + jnp.log(lax.optimization_barrier(jnp.sum(jnp.exp(logits - row_max[:, None]), axis=1)))
    target_logit = jnp.take_along_axis(logits, target_ids[:, None].astype(jnp.int32), axis=1)[:, 0]
    valid_count = jnp.sum(weight_rows)
    mean_loss = jnp.sum((log_total - target_logit) * weight_rows) / valid_count
    prob_rows = jnp.exp(logits - log_total[:, None])
    onehot = (jnp.arange(V, dtype=jnp.int32)[None, :] == target_ids[:, None]).astype(jnp.float32)
    grad_scale = weight_rows * (loss_scale / valid_count)
    grad_logits = ((prob_rows - onehot) * grad_scale[:, None]).astype(jnp.bfloat16)
    hidden_grad = jnp.dot(grad_logits, head_weight.T, preferred_element_type=jnp.float32).astype(jnp.bfloat16)

    def block_grad(columns):
        return jnp.dot(hidden.T, columns, preferred_element_type=jnp.float32).astype(jnp.bfloat16)
    stacked = lax.map(block_grad, grad_logits.reshape(TOKENS, blocks, block_cols).transpose(1, 0, 2))
    head_grad = stacked.transpose(1, 0, 2).reshape(D, V)
    return (mean_loss, head_grad, hidden_grad)
```

```python
import functools

import jax
import jax.numpy as jnp
from jax import lax
from jax.experimental import pallas as pl
from jax.experimental.pallas import tpu as pltpu
from jax.sharding import PartitionSpec as P

VALID_MOST = 32
MESH = pl.DeviceIdType.MESH
VMEM = pl.BlockSpec(memory_space=pltpu.VMEM)
SMEM = pl.BlockSpec(memory_space=pltpu.SMEM)
F32 = jnp.float32
BF16 = jnp.bfloat16


def remote(src, dst, send_sem, recv_sem, where):
    return pltpu.make_async_remote_copy(
        src_ref=src, dst_ref=dst, send_sem=send_sem, recv_sem=recv_sem, device_id=where, device_id_type=MESH
    )


def greet(where):
    pl.semaphore_signal(pltpu.get_barrier_semaphore(), inc=1, device_id=where, device_id_type=MESH)


def gather_kernel(n_dp, hidden, targets, mask, docs, rows, meta_out, meta, merged, row_s, row_r, fwd_s, fwd_r, meta_s, meta_r):
    d, v = lax.axis_index("dp"), lax.axis_index("vocab")
    core = lax.rem(v, 2)
    partner = (d, v + 1 - 2 * core)
    peers = [lax.rem(d + k, n_dp) for k in range(n_dp)]
    for k in range(1, n_dp):
        greet((peers[k], v))
    greet(partner)

    tok = hidden.shape[0]
    half = VALID_MOST // 2
    u = lax.broadcasted_iota(jnp.int32, (tok, tok), 0)
    t = lax.broadcasted_iota(jnp.int32, (tok, tok), 1)
    mask_f = jnp.broadcast_to(mask[...].astype(F32), (8, tok))
    docs_f = jnp.broadcast_to(docs[...].astype(F32), (8, tok))
    upto = jnp.where(u <= t, 1.0, 0.0).astype(BF16)
    after = jnp.where(u == t + 1, 1.0, 0.0).astype(BF16)
    rank = jnp.dot(mask_f.astype(BF16), upto, preferred_element_type=F32)[0:1] - 1.0
    following = jnp.dot(docs_f.astype(BF16), after, preferred_element_type=F32)[0:1]
    mask_f, docs_f = mask_f[0:1], docs_f[0:1]
    slot = lax.broadcasted_iota(jnp.int32, (VALID_MOST, tok), 0).astype(F32)
    chosen = jnp.where(slot == rank, 1.0, 0.0) * mask_f
    picked = jnp.dot(chosen.astype(BF16), hidden[...], preferred_element_type=F32).astype(BF16)
    rows[d, 0] = picked[:half]
    rows[d, 1] = picked[half:]
    place = lax.broadcasted_iota(jnp.int32, (1, tok), 1)
    inner = jnp.where(place < tok - 1, 1.0, 0.0)
    same = jnp.where(following == docs_f, 1.0, 0.0) * inner

    def column(values):
        return jnp.sum(chosen * values, axis=1, keepdims=True)

    fields = [
        column(targets[...].astype(F32)),
        column(same),
        column((place + d * tok).astype(F32)),
        jnp.broadcast_to(docs_f[:, 0:1], (VALID_MOST, 1)),
        column(1.0 - inner),
        jnp.broadcast_to(docs_f[:, tok - 1 : tok], (VALID_MOST, 1)),
    ]
    lane = lax.broadcasted_iota(jnp.int32, (VALID_MOST, 128), 1)
    packed = jnp.zeros((VALID_MOST, 128), F32)
    for number, field in enumerate(fields):
        packed = jnp.where(lane == number, field, packed)
    meta[d] = packed

    pl.semaphore_wait(pltpu.get_barrier_semaphore(), n_dp)
    sends = []
    for k in range(1, n_dp):
        sends.append(remote(rows.at[d, core], rows.at[d, core], row_s.at[k], row_r.at[k], (peers[k], v)))
        sends.append(remote(meta.at[d], meta.at[d], meta_s.at[k], meta_r.at[k], (peers[k], v)))
    for copy in sends:
        copy.start()
    forwards = []
    for k in range(1, n_dp):
        source = lax.rem(d + n_dp - k, n_dp)
        block = rows.at[source, core]
        remote(block, block, row_s.at[k], row_r.at[k], (peers[k], v)).wait_recv()
        copy = remote(block, block, fwd_s.at[k], fwd_r.at[k], partner)
        copy.start()
        forwards.append(copy)
    for k in range(1, n_dp):
        source = lax.rem(d + n_dp - k, n_dp)
        remote(meta.at[source], meta.at[source], meta_s.at[k], meta_r.at[k], (peers[k], v)).wait_recv()
    for group in range(n_dp):
        block = meta[group]
        valid = block[:, 1:2]
        if group < n_dp - 1:
            first = meta[group + 1][:, 3:4]
            valid = valid + block[:, 4:5] * jnp.where(block[:, 5:6] == first, 1.0, 0.0)
        merged[group * VALID_MOST : (group + 1) * VALID_MOST] = jnp.where(lane == 1, valid, block)
    meta_out[...] = merged[...].T[:8]
    for k in range(1, n_dp):
        source = lax.rem(d + n_dp - k, n_dp)
        other = rows.at[source, 1 - core]
        remote(other, other, fwd_s.at[k], fwd_r.at[k], partner).wait_recv()
    for copy in sends + forwards:
        copy.wait_send()


def gather_rows(n_dp, hidden, targets, mask, docs):
    width = hidden.shape[1]
    dma = pltpu.SemaphoreType.DMA((n_dp,))
    total = n_dp * VALID_MOST
    return pl.pallas_call(
        functools.partial(gather_kernel, n_dp),
        out_shape=(
            jax.ShapeDtypeStruct((n_dp, 2, VALID_MOST // 2, width), BF16),
            jax.ShapeDtypeStruct((8, total), F32),
        ),
        in_specs=[VMEM] * 4,
        out_specs=(VMEM, VMEM),
        scratch_shapes=[pltpu.VMEM((n_dp, VALID_MOST, 128), F32), pltpu.VMEM((total, 128), F32)] + [dma] * 6,
        compiler_params=pltpu.CompilerParams(collective_id=0, has_side_effects=True),
    )(hidden, targets[None], mask[None], docs[None])


def stats_kernel(n_dp, n_v, top, total, hit, meta, scale, out, slots, send, recv):
    d, v = lax.axis_index("dp"), lax.axis_index("vocab")
    me = d * n_v + v
    count = n_dp * n_v

    def device(k):
        index = lax.rem(me + k, count)
        return (index // n_v, lax.rem(index, n_v))

    def hello(k, carry):
        greet(device(k))
        return carry

    lax.fori_loop(1, count, hello, 0)
    line = lax.broadcasted_iota(jnp.int32, slots.shape[1:], 0)
    slots[me] = jnp.where(line == 0, top[...], jnp.where(line == 1, total[...], hit[...]))
    pl.semaphore_wait(pltpu.get_barrier_semaphore(), count - 1)

    def push(k, carry):
        remote(slots.at[me], slots.at[me], send.at[k], recv.at[k], device(k)).start()
        return carry

    lax.fori_loop(1, count, push, 0)

    def arrive(k, carry):
        source = slots.at[lax.rem(me + count - k, count)]
        copy = remote(source, source, send.at[k], recv.at[k], device(k))
        copy.wait_recv()
        copy.wait_send()
        return carry

    lax.fori_loop(1, count, arrive, 0)
    every = slots[...]
    row_max = jnp.max(every, axis=0)[0:1]
    row_total = jnp.sum(every[:, 1:2, :] * jnp.exp(every[:, 0:1, :] - row_max), axis=0)
    target_logit = jnp.sum(every, axis=0)[2:3]
    log_total = row_max + jnp.log(row_total)
    weight = meta[1:2, :]
    valid_count = jnp.sum(weight, axis=1, keepdims=True)
    mean_loss = jnp.sum((log_total - target_logit) * weight, axis=1, keepdims=True) / valid_count
    grad_scale = weight * (scale[0, 0] / valid_count)
    out[...] = jnp.where(line == 0, log_total, jnp.where(line == 1, grad_scale, mean_loss))


def share_stats(n_dp, n_v, top, total, hit, meta, scale):
    count = n_dp * n_v
    rows = top.shape[0]
    dma = pltpu.SemaphoreType.DMA((count,))
    return pl.pallas_call(
        functools.partial(stats_kernel, n_dp, n_v),
        out_shape=jax.ShapeDtypeStruct((8, rows), F32),
        in_specs=[VMEM] * 4 + [SMEM],
        out_specs=VMEM,
        scratch_shapes=[pltpu.VMEM((count, 8, rows), F32), dma, dma],
        compiler_params=pltpu.CompilerParams(collective_id=1, has_side_effects=True),
    )(top[None], total[None], hit[None], meta, scale.reshape(1, 1))


def scatter_kernel(n_dp, n_z, term, meta, out, got1, sum1, got2, sum2, got3, s1, r1, s2, r2, s3, r3):
    d, v = lax.axis_index("dp"), lax.axis_index("vocab")
    z, core = v // 2, lax.rem(v, 2)
    partner = (d, v + 1 - 2 * core)
    peers = [lax.rem(d + k, n_dp) for k in range(n_dp)]
    greet(partner)
    for k in range(1, n_dp):
        greet((peers[k], v))

    def along(step):
        return lax.rem(z + step, n_z)

    def hello(step, carry):
        greet((d, 2 * along(step) + core))
        return carry

    lax.fori_loop(1, n_z, hello, 0)
    pl.semaphore_wait(pltpu.get_barrier_semaphore(), n_dp + n_z - 1)

    order = list(range(1, n_dp)) + [0]

    def first(k):
        return remote(term.at[peers[k], :, 1 - core], got1.at[peers[k]], s1.at[k], r1.at[k], partner)

    def second(k, step):
        at = along(step)
        return remote(sum1.at[peers[k], at], got2.at[k, at], s2.at[k, step], r2.at[k, step], (peers[k], v))

    def third(step):
        at = along(step)
        return remote(sum2.at[at], got3.at[step], s3.at[step], r3.at[step], (d, 2 * at + core))

    for k in order:
        first(k).start()
    for k in order:
        first(k).wait_recv()

        def combine(step, carry, k=k):
            at = along(step)
            sum1[peers[k], at] = term[peers[k], at, core] + got1[peers[k], at]
            if k:
                second(k, step).start()
            return carry

        lax.fori_loop(1, n_z + 1, combine, 0)

    def merge(step, carry):
        at = along(step)
        value = sum1[d, at]
        for k in range(1, n_dp):
            second(k, step).wait_recv()
            value = value + got2[k, at]
        sum2[at] = value
        return carry

    def forward(step, carry):
        merge(step, 0)
        third(step).start()
        return carry

    lax.fori_loop(1, n_z, forward, 0)
    merge(n_z, 0)

    def finish(step, value):
        third(step).wait_recv()
        return value + got3[step]

    value = lax.fori_loop(1, n_z, finish, sum2[z])
    tokens = out.shape[0]
    spot = lax.broadcasted_iota(jnp.int32, (tokens, value.shape[1]), 0).astype(F32)
    onehot = jnp.where(spot == meta[2:3, :], 1.0, 0.0).astype(BF16)
    high = value.astype(BF16)
    rest = value - high.astype(F32)
    middle = rest.astype(BF16)
    low = (rest - middle.astype(F32)).astype(BF16)
    placed = jnp.zeros(out.shape, F32)
    for part in (low, middle, high):
        placed = placed + lax.dot_general(onehot, part, (((1,), (1,)), ((), ())), preferred_element_type=F32)
    out[...] = placed.astype(BF16)

    for k in order:
        first(k).wait_send()

    def drain2(step, carry):
        for k in range(1, n_dp):
            second(k, step).wait_send()
        return carry

    def drain3(step, carry):
        third(step).wait_send()
        return carry

    lax.fori_loop(1, n_z + 1, drain2, 0)
    lax.fori_loop(1, n_z, drain3, 0)


def scatter_terms(n_dp, n_v, term, meta, tokens):
    n_z = n_v // 2
    own, rows = term.shape[0] // (n_dp * n_v), term.shape[1]
    dma = pltpu.SemaphoreType.DMA
    return pl.pallas_call(
        functools.partial(scatter_kernel, n_dp, n_z),
        out_shape=jax.ShapeDtypeStruct((tokens, own), BF16),
        in_specs=[VMEM] * 2,
        out_specs=VMEM,
        scratch_shapes=[
            pltpu.VMEM((n_dp, n_z, own, rows), F32),
            pltpu.VMEM((n_dp, n_z, own, rows), F32),
            pltpu.VMEM((n_dp, n_z, own, rows), F32),
            pltpu.VMEM((n_z, own, rows), F32),
            pltpu.VMEM((n_z, own, rows), F32),
            dma((n_dp,)),
            dma((n_dp,)),
            dma((n_dp, n_z + 1)),
            dma((n_dp, n_z + 1)),
            dma((n_z,)),
            dma((n_z,)),
        ],
        compiler_params=pltpu.CompilerParams(collective_id=2, has_side_effects=True),
    )(term.reshape(n_dp, n_z, 2, own, rows), meta)


def on_device(n_dp, n_v, hidden, head_weight, target_ids, loss_mask, doc_ids, loss_scale):
    width, block_cols = head_weight.shape
    rows, meta = gather_rows(n_dp, hidden, target_ids, loss_mask, doc_ids)
    rows_all = rows.reshape(n_dp * VALID_MOST, width)
    col_base = lax.axis_index(("dp", "vocab")) * block_cols
    shifted_ids = meta[0].astype(jnp.int32) - col_base
    logits = jnp.dot(rows_all, head_weight, preferred_element_type=F32)
    local_max = jnp.max(logits, axis=1)
    onehot = jnp.arange(block_cols, dtype=jnp.int32)[None, :] == shifted_ids[:, None]
    target_part = jnp.sum(jnp.where(onehot, logits, 0.0), axis=1)
    local_sum = jnp.sum(jnp.exp(logits - local_max[:, None]), axis=1)
    stats = share_stats(n_dp, n_v, local_max, local_sum, target_part, meta, loss_scale)
    log_total, grad_scale, mean_loss = stats[0], stats[1], stats[2, 0]
    prob_rows = jnp.exp(logits - log_total[:, None])
    grad_logits = ((prob_rows - onehot.astype(F32)) * grad_scale[:, None]).astype(BF16)
    term = lax.dot_general(head_weight, grad_logits, (((1,), (1,)), ((), ())), preferred_element_type=F32)
    hidden_grad = scatter_terms(n_dp, n_v, term, meta, hidden.shape[0] * n_dp)
    head_grad = lax.dot_general(rows_all, grad_logits, (((0,), (0,)), ((), ())), preferred_element_type=F32).astype(BF16)
    return (mean_loss, head_grad, hidden_grad)


def solution(mesh):
    return jax.shard_map(
        functools.partial(on_device, mesh.shape["dp"], mesh.shape["vocab"]),
        mesh=mesh,
        in_specs=(P("dp", None), P(None, ("dp", "vocab")), P("dp"), P("dp"), P("dp"), P()),
        out_specs=(P(), P(None, ("dp", "vocab")), P(None, ("dp", "vocab"))),
        check_vma=False,
    )
```

```python
import functools

import jax
import jax.numpy as jnp
from jax import lax
from jax.experimental import pallas as pl
from jax.experimental.pallas import tpu as pltpu
from jax.sharding import PartitionSpec as P

VALID_MOST = 32
MESH = pl.DeviceIdType.MESH
VMEM = pl.BlockSpec(memory_space=pltpu.VMEM)
SMEM = pl.BlockSpec(memory_space=pltpu.SMEM)
F32 = jnp.float32
BF16 = jnp.bfloat16


def remote(src, dst, send_sem, recv_sem, where):
    return pltpu.make_async_remote_copy(
        src_ref=src, dst_ref=dst, send_sem=send_sem, recv_sem=recv_sem, device_id=where, device_id_type=MESH
    )


def greet(where):
    pl.semaphore_signal(pltpu.get_barrier_semaphore(), inc=1, device_id=where, device_id_type=MESH)


def gather_kernel(n_dp, hidden, targets, mask, docs, rows, meta_out, meta, merged, row_s, row_r, fwd_s, fwd_r, meta_s, meta_r):
    d, v = lax.axis_index("dp"), lax.axis_index("vocab")
    core = lax.rem(v, 2)
    partner = (d, v + 1 - 2 * core)
    peers = [lax.rem(d + k, n_dp) for k in range(n_dp)]
    for k in range(1, n_dp):
        greet((peers[k], v))
    greet(partner)

    tok = hidden.shape[0]
    half = VALID_MOST // 2
    u = lax.broadcasted_iota(jnp.int32, (tok, tok), 0)
    t = lax.broadcasted_iota(jnp.int32, (tok, tok), 1)
    mask_f = jnp.broadcast_to(mask[...].astype(F32), (8, tok))
    docs_f = jnp.broadcast_to(docs[...].astype(F32), (8, tok))
    upto = jnp.where(u <= t, 1.0, 0.0).astype(BF16)
    after = jnp.where(u == t + 1, 1.0, 0.0).astype(BF16)
    rank = jnp.dot(mask_f.astype(BF16), upto, preferred_element_type=F32)[0:1] - 1.0
    following = jnp.dot(docs_f.astype(BF16), after, preferred_element_type=F32)[0:1]
    mask_f, docs_f = mask_f[0:1], docs_f[0:1]
    slot = lax.broadcasted_iota(jnp.int32, (VALID_MOST, tok), 0).astype(F32)
    chosen = jnp.where(slot == rank, 1.0, 0.0) * mask_f
    picked = jnp.dot(chosen.astype(BF16), hidden[...], preferred_element_type=F32).astype(BF16)
    rows[d, 0] = picked[:half]
    rows[d, 1] = picked[half:]
    place = lax.broadcasted_iota(jnp.int32, (1, tok), 1)
    inner = jnp.where(place < tok - 1, 1.0, 0.0)
    same = jnp.where(following == docs_f, 1.0, 0.0) * inner

    def column(values):
        return jnp.sum(chosen * values, axis=1, keepdims=True)

    fields = [
        column(targets[...].astype(F32)),
        column(same),
        column((place + d * tok).astype(F32)),
        jnp.broadcast_to(docs_f[:, 0:1], (VALID_MOST, 1)),
        column(1.0 - inner),
        jnp.broadcast_to(docs_f[:, tok - 1 : tok], (VALID_MOST, 1)),
    ]
    lane = lax.broadcasted_iota(jnp.int32, (VALID_MOST, 128), 1)
    packed = jnp.zeros((VALID_MOST, 128), F32)
    for number, field in enumerate(fields):
        packed = jnp.where(lane == number, field, packed)
    meta[d] = packed

    pl.semaphore_wait(pltpu.get_barrier_semaphore(), n_dp)
    sends = []
    for k in range(1, n_dp):
        sends.append(remote(rows.at[d, core], rows.at[d, core], row_s.at[k], row_r.at[k], (peers[k], v)))
        sends.append(remote(meta.at[d], meta.at[d], meta_s.at[k], meta_r.at[k], (peers[k], v)))
    for copy in sends:
        copy.start()
    forwards = []
    for k in range(1, n_dp):
        source = lax.rem(d + n_dp - k, n_dp)
        block = rows.at[source, core]
        remote(block, block, row_s.at[k], row_r.at[k], (peers[k], v)).wait_recv()
        copy = remote(block, block, fwd_s.at[k], fwd_r.at[k], partner)
        copy.start()
        forwards.append(copy)
    for k in range(1, n_dp):
        source = lax.rem(d + n_dp - k, n_dp)
        remote(meta.at[source], meta.at[source], meta_s.at[k], meta_r.at[k], (peers[k], v)).wait_recv()
    for group in range(n_dp):
        block = meta[group]
        valid = block[:, 1:2]
        if group < n_dp - 1:
            first = meta[group + 1][:, 3:4]
            valid = valid + block[:, 4:5] * jnp.where(block[:, 5:6] == first, 1.0, 0.0)
        merged[group * VALID_MOST : (group + 1) * VALID_MOST] = jnp.where(lane == 1, valid, block)
    meta_out[...] = merged[...].T[:8]
    for k in range(1, n_dp):
        source = lax.rem(d + n_dp - k, n_dp)
        other = rows.at[source, 1 - core]
        remote(other, other, fwd_s.at[k], fwd_r.at[k], partner).wait_recv()
    for copy in sends + forwards:
        copy.wait_send()


def gather_rows(n_dp, hidden, targets, mask, docs):
    width = hidden.shape[1]
    dma = pltpu.SemaphoreType.DMA((n_dp,))
    total = n_dp * VALID_MOST
    return pl.pallas_call(
        functools.partial(gather_kernel, n_dp),
        out_shape=(
            jax.ShapeDtypeStruct((n_dp, 2, VALID_MOST // 2, width), BF16),
            jax.ShapeDtypeStruct((8, total), F32),
        ),
        in_specs=[VMEM] * 4,
        out_specs=(VMEM, VMEM),
        scratch_shapes=[pltpu.VMEM((n_dp, VALID_MOST, 128), F32), pltpu.VMEM((total, 128), F32)] + [dma] * 6,
        compiler_params=pltpu.CompilerParams(collective_id=0, has_side_effects=True),
    )(hidden, targets[None], mask[None], docs[None])


def stats_kernel(n_dp, n_v, top, total, hit, meta, scale, out, slots, send, recv):
    d, v = lax.axis_index("dp"), lax.axis_index("vocab")
    me = d * n_v + v
    count = n_dp * n_v

    def device(k):
        index = lax.rem(me + k, count)
        return (index // n_v, lax.rem(index, n_v))

    def hello(k, carry):
        greet(device(k))
        return carry

    lax.fori_loop(1, count, hello, 0)
    line = lax.broadcasted_iota(jnp.int32, slots.shape[1:], 0)
    slots[me] = jnp.where(line == 0, top[...], jnp.where(line == 1, total[...], hit[...]))
    pl.semaphore_wait(pltpu.get_barrier_semaphore(), count - 1)

    def push(k, carry):
        remote(slots.at[me], slots.at[me], send.at[k], recv.at[k], device(k)).start()
        return carry

    lax.fori_loop(1, count, push, 0)

    def arrive(k, carry):
        source = slots.at[lax.rem(me + count - k, count)]
        copy = remote(source, source, send.at[k], recv.at[k], device(k))
        copy.wait_recv()
        copy.wait_send()
        return carry

    lax.fori_loop(1, count, arrive, 0)
    every = slots[...]
    row_max = jnp.max(every, axis=0)[0:1]
    row_total = jnp.sum(every[:, 1:2, :] * jnp.exp(every[:, 0:1, :] - row_max), axis=0)
    target_logit = jnp.sum(every, axis=0)[2:3]
    log_total = row_max + jnp.log(row_total)
    weight = meta[1:2, :]
    valid_count = jnp.sum(weight, axis=1, keepdims=True)
    mean_loss = jnp.sum((log_total - target_logit) * weight, axis=1, keepdims=True) / valid_count
    grad_scale = weight * (scale[0, 0] / valid_count)
    out[...] = jnp.where(line == 0, log_total, jnp.where(line == 1, grad_scale, mean_loss))


def share_stats(n_dp, n_v, top, total, hit, meta, scale):
    count = n_dp * n_v
    rows = top.shape[0]
    dma = pltpu.SemaphoreType.DMA((count,))
    return pl.pallas_call(
        functools.partial(stats_kernel, n_dp, n_v),
        out_shape=jax.ShapeDtypeStruct((8, rows), F32),
        in_specs=[VMEM] * 4 + [SMEM],
        out_specs=VMEM,
        scratch_shapes=[pltpu.VMEM((count, 8, rows), F32), dma, dma],
        compiler_params=pltpu.CompilerParams(collective_id=1, has_side_effects=True),
    )(top[None], total[None], hit[None], meta, scale.reshape(1, 1))


def scatter_kernel(n_dp, n_z, weight, grads_t, meta, out, grads, panels, fetched, term, got1, sum1, got2, sum2, got3, s1, r1, s2, r2, s3, r3):
    d, v = lax.axis_index("dp"), lax.axis_index("vocab")
    z, core = v // 2, lax.rem(v, 2)
    partner = (d, v + 1 - 2 * core)
    peers = [lax.rem(d + k, n_dp) for k in range(n_dp)]
    order = list(range(1, n_dp)) + [0]
    slots, _, chunk = panels.shape
    own = term.shape[3]
    parts = weight.shape[1] // n_dp // chunk
    steps = [(k, part) for k in order for part in range(parts)]

    def fetch(number):
        k, part = steps[number]
        start = pl.multiple_of((peers[k] * parts + part) * chunk, chunk)
        slot = number % slots
        return pltpu.make_async_copy(weight.at[:, pl.ds(start, chunk)], panels.at[slot], fetched.at[slot])

    for number in range(slots):
        fetch(number).start()
    greet(partner)
    for k in range(1, n_dp):
        greet((peers[k], v))

    def along(step):
        return lax.rem(z + step, n_z)

    def hello(step, carry):
        greet((d, 2 * along(step) + core))
        return carry

    lax.fori_loop(1, n_z, hello, 0)

    def first(k):
        return remote(term.at[peers[k], :, 1 - core], got1.at[peers[k]], s1.at[k], r1.at[k], partner)

    def second(k, step):
        at = along(step)
        return remote(sum1.at[peers[k], at], got2.at[k, at], s2.at[k, step], r2.at[k, step], (peers[k], v))

    def third(step):
        at = along(step)
        return remote(sum2.at[at], got3.at[step], s3.at[step], r3.at[step], (d, 2 * at + core))

    grads[...] = grads_t[...].T

    def multiply(number):
        k, part = steps[number]
        slot = number % slots
        fetch(number).wait()
        tile = min(256, chunk)

        def column(j, carry):
            panel = panels[slot, :, pl.ds(pl.multiple_of(j * tile, tile), tile)]
            block = jnp.dot(grads[...], panel, preferred_element_type=F32).T
            deep = tile // (2 * own)
            base = part * (chunk // (2 * own)) + j * deep
            term[peers[k], pl.ds(base, deep)] = block.reshape(deep, 2, own, block.shape[1])
            return carry

        lax.fori_loop(0, chunk // tile, column, 0)
        if number + slots < len(steps):
            fetch(number + slots).start()

    def join(k):
        first(k).wait_recv()

        def combine(step, carry):
            at = along(step)
            sum1[peers[k], at] = term[peers[k], at, core] + got1[peers[k], at]
            if k:
                second(k, step).start()
            return carry

        lax.fori_loop(1, n_z + 1, combine, 0)

    for number, (k, part) in enumerate(steps):
        multiply(number)
        if number == 0:
            pl.semaphore_wait(pltpu.get_barrier_semaphore(), n_dp + n_z - 1)
        if part == parts - 1:
            first(k).start()
        if part == 0 and number:
            join(steps[number - 1][0])
    join(order[-1])

    def merge(step, carry):
        at = along(step)
        value = sum1[d, at]
        for k in range(1, n_dp):
            second(k, step).wait_recv()
            value = value + got2[k, at]
        sum2[at] = value
        return carry

    def forward(step, carry):
        merge(step, 0)
        third(step).start()
        return carry

    lax.fori_loop(1, n_z, forward, 0)
    merge(n_z, 0)

    def finish(step, value):
        third(step).wait_recv()
        return value + got3[step]

    value = lax.fori_loop(1, n_z, finish, sum2[z])
    tokens = out.shape[0]
    spot = lax.broadcasted_iota(jnp.int32, (tokens, value.shape[1]), 0).astype(F32)
    onehot = jnp.where(spot == meta[2:3, :], 1.0, 0.0).astype(BF16)
    high = value.astype(BF16)
    rest = value - high.astype(F32)
    middle = rest.astype(BF16)
    low = (rest - middle.astype(F32)).astype(BF16)
    placed = jnp.zeros(out.shape, F32)
    for part in (low, middle, high):
        placed = placed + lax.dot_general(onehot, part, (((1,), (1,)), ((), ())), preferred_element_type=F32)
    out[...] = placed.astype(BF16)

    for k in order:
        first(k).wait_send()

    def drain2(step, carry):
        for k in range(1, n_dp):
            second(k, step).wait_send()
        return carry

    def drain3(step, carry):
        third(step).wait_send()
        return carry

    lax.fori_loop(1, n_z + 1, drain2, 0)
    lax.fori_loop(1, n_z, drain3, 0)


def scatter_terms(n_dp, n_v, weight, grads, meta, tokens):
    n_z = n_v // 2
    columns, width = weight.shape
    own, rows = width // (n_dp * n_v), grads.shape[1]
    chunk = width // n_dp // 2
    dma = pltpu.SemaphoreType.DMA
    return pl.pallas_call(
        functools.partial(scatter_kernel, n_dp, n_z),
        out_shape=jax.ShapeDtypeStruct((tokens, own), BF16),
        in_specs=[pl.BlockSpec(memory_space=pl.ANY), VMEM, VMEM],
        out_specs=VMEM,
        scratch_shapes=[
            pltpu.VMEM((rows, columns), BF16),
            pltpu.VMEM((4, columns, chunk), BF16),
            dma((4,)),
            pltpu.VMEM((n_dp, n_z, 2, own, rows), F32),
            pltpu.VMEM((n_dp, n_z, own, rows), F32),
            pltpu.VMEM((n_dp, n_z, own, rows), F32),
            pltpu.VMEM((n_dp, n_z, own, rows), F32),
            pltpu.VMEM((n_z, own, rows), F32),
            pltpu.VMEM((n_z, own, rows), F32),
            dma((n_dp,)),
            dma((n_dp,)),
            dma((n_dp, n_z + 1)),
            dma((n_dp, n_z + 1)),
            dma((n_z,)),
            dma((n_z,)),
        ],
        compiler_params=pltpu.CompilerParams(collective_id=2, has_side_effects=True, vmem_limit_bytes=40 * 1024 * 1024),
    )(weight, grads, meta)


def on_device(n_dp, n_v, hidden, head_weight, target_ids, loss_mask, doc_ids, loss_scale):
    width, block_cols = head_weight.shape
    rows, meta = gather_rows(n_dp, hidden, target_ids, loss_mask, doc_ids)
    rows_all = rows.reshape(n_dp * VALID_MOST, width)
    col_base = lax.axis_index(("dp", "vocab")) * block_cols
    shifted_ids = meta[0].astype(jnp.int32) - col_base
    logits = jnp.dot(rows_all, head_weight, preferred_element_type=F32)
    local_max = jnp.max(logits, axis=1)
    onehot = jnp.arange(block_cols, dtype=jnp.int32)[None, :] == shifted_ids[:, None]
    target_part = jnp.sum(jnp.where(onehot, logits, 0.0), axis=1)
    local_sum = jnp.sum(jnp.exp(logits - local_max[:, None]), axis=1)
    stats = share_stats(n_dp, n_v, local_max, local_sum, target_part, meta, loss_scale)
    log_total, grad_scale, mean_loss = stats[0], stats[1], stats[2, 0]
    prob_rows = jnp.exp(logits - log_total[:, None])
    grad_logits = ((prob_rows - onehot.astype(F32)) * grad_scale[:, None]).astype(BF16)
    hidden_grad = scatter_terms(n_dp, n_v, head_weight.T, grad_logits.T, meta, hidden.shape[0] * n_dp)
    head_grad = lax.dot_general(rows_all, grad_logits, (((0,), (0,)), ((), ())), preferred_element_type=F32).astype(BF16)
    return (mean_loss, head_grad, hidden_grad)


def solution(mesh):
    return jax.shard_map(
        functools.partial(on_device, mesh.shape["dp"], mesh.shape["vocab"]),
        mesh=mesh,
        in_specs=(P("dp", None), P(None, ("dp", "vocab")), P("dp"), P("dp"), P("dp"), P()),
        out_specs=(P(), P(None, ("dp", "vocab")), P(None, ("dp", "vocab"))),
        check_vma=False,
    )
```
